32 devices in a mesh: dp: 1 (over z), ep: 32 (over y, x, core).
Axes of the slice: x: 4, y: 4, z: 1, core: 2. Of those that a mesh axis runs over, the one named last changes fastest.
The devices are a block of a 4x4x8 slice.
Arguments:
- x: bfloat16 [16384, 1536], P(('dp', 'ep'))
- route_idx: int32 [16384, 8], P(('dp', 'ep'))
- route_gate: float32 [16384, 8], P(('dp', 'ep'))
- w_gate: bfloat16 [32, 1536, 512], P('ep')
- w_up: bfloat16 [32, 1536, 512], P('ep')
- w_down: bfloat16 [32, 512, 1536], P('ep')
- grad_y: bfloat16 [16384, 1536], P(('dp', 'ep'))
Outputs:
- output 1: bfloat16 [16384, 1536], P(('dp', 'ep'))
- output 2: bfloat16 [16384, 1536], P(('dp', 'ep'))
- output 3: bfloat16 [32, 1536, 512], P(('dp', 'ep'))
- output 4: bfloat16 [32, 1536, 512], P(('dp', 'ep'))
- output 5: bfloat16 [32, 512, 1536], P(('dp', 'ep'))
All inputs are finite; a program needn't handle non-finite values.
Results may differ from the reference program's by a relative error of at most 0.00143.
Values are sent between devices in bfloat16 or wider.
A program may use at most 768 MiB of HBM per device.

```python
import jax
import jax.numpy as jnp
from jax import lax

GROUP_SIZE = 32
TOKENS = 512
D_MODEL = 1536
D_FF = 512
TOP_K = 8
ROW_BLOCK = 64
CAPACITY = 3 * TOKENS // 4
T_ALL = GROUP_SIZE * TOKENS


def draw_routes(route_key):
    order_key, src_key = jax.random.split(route_key)
    expert_order = jax.random.permutation(order_key, GROUP_SIZE).astype(jnp.int32)
    hot_count = TOP_K // 2
    cold_count = GROUP_SIZE - hot_count
    spare = TOP_K * TOKENS - hot_count * CAPACITY - cold_count
    slot_ids = jnp.arange(TOP_K * TOKENS, dtype=jnp.int32)

    def one_source(one_key):
        unit_key, row_key = jax.random.split(one_key)
        units = jax.random.permutation(unit_key, cold_count * (CAPACITY - 1))[:spare] // (CAPACITY - 1)
        cold_load = 1 + jnp.bincount(units, length=cold_count)
        loads = jnp.concatenate([jnp.full((hot_count,), CAPACITY, jnp.int32), cold_load.astype(jnp.int32)])
        run_ends = jnp.cumsum(loads)
        run_index = jnp.searchsorted(run_ends, slot_ids, side="right")
        grid = expert_order[run_index].reshape(TOP_K, TOKENS).T
        return grid[jax.random.permutation(row_key, TOKENS)]

    return jax.vmap(one_source)(jax.random.split(src_key, GROUP_SIZE)).reshape(T_ALL, TOP_K)


def setup_inputs(seed: int = 0, part: int = 0) -> dict:
    part_key = jax.random.fold_in(jax.random.key(seed), part)
    x_key, gate_key, grad_key, route_key = jax.random.split(part_key, 4)
    wg_key, wu_key, wd_key = jax.random.split(jax.random.key(seed + 1), 3)
    x = jax.random.normal(x_key, (T_ALL, D_MODEL), jnp.float32).astype(jnp.bfloat16)
    route_gate = jax.random.uniform(gate_key, (T_ALL, TOP_K), jnp.float32, 0.3, 0.7)
    grad_y = jax.random.normal(grad_key, (T_ALL, D_MODEL), jnp.float32).astype(jnp.bfloat16)
    w_gate = (jax.random.normal(wg_key, (GROUP_SIZE, D_MODEL, D_FF), jnp.float32) * D_MODEL ** -0.5).astype(jnp.bfloat16)
    w_up = (jax.random.normal(wu_key, (GROUP_SIZE, D_MODEL, D_FF), jnp.float32) * D_MODEL ** -0.5).astype(jnp.bfloat16)
    w_down = (jax.random.normal(wd_key, (GROUP_SIZE, D_FF, D_MODEL), jnp.float32) * D_FF ** -0.5).astype(jnp.bfloat16)
    return {"x": x, "route_idx": draw_routes(route_key), "route_gate": route_gate, "w_gate": w_gate, "w_up": w_up, "w_down": w_down, "grad_y": grad_y}


def expert_block(rows, out_cot, gate_mat, up_mat, down_mat):
    pre_gate = jnp.dot(rows, gate_mat, preferred_element_type=jnp.float32)
    pre_up = jnp.dot(rows, up_mat, preferred_element_type=jnp.float32)
    sig_gate = jax.nn.sigmoid(pre_gate)
    hidden = (pre_gate * sig_gate * pre_up).astype(jnp.bfloat16)
    expert_out = jnp.dot(hidden, down_mat, preferred_element_type=jnp.float32).astype(jnp.bfloat16)
    grad_hidden = jnp.dot(out_cot, down_mat.T, preferred_element_type=jnp.float32).astype(jnp.bfloat16).astype(jnp.float32)
    grad_gate = (grad_hidden * pre_up * (sig_gate * (1.0 + pre_gate * (1.0 - sig_gate)))).astype(jnp.bfloat16)
    grad_up = (grad_hidden * (pre_gate * sig_gate)).astype(jnp.bfloat16)
    grad_rows = (jnp.dot(grad_gate, gate_mat.T, preferred_element_type=jnp.float32) + jnp.dot(grad_up, up_mat.T, preferred_element_type=jnp.float32)).astype(jnp.bfloat16)
    grad_gate_mat = jnp.dot(rows.T, grad_gate, preferred_element_type=jnp.float32)
    grad_up_mat = jnp.dot(rows.T, grad_up, preferred_element_type=jnp.float32)
    grad_down_mat = jnp.dot(hidden.T, out_cot, preferred_element_type=jnp.float32)
    return expert_out, grad_rows, grad_gate_mat, grad_up_mat, grad_down_mat


def reference(x, route_idx, route_gate, w_gate, w_up, w_down, grad_y):
    n_slots = T_ALL * TOP_K
    n_blocks = n_slots // ROW_BLOCK + GROUP_SIZE
    flat_exp = route_idx.reshape(n_slots)
    order = jnp.argsort(flat_exp, stable=True).astype(jnp.int32)
    sorted_exp = flat_exp[order]
    exp_counts = jnp.bincount(flat_exp, length=GROUP_SIZE).astype(jnp.int32)
    exp_starts = jnp.cumsum(exp_counts) - exp_counts
    padded = (exp_counts + ROW_BLOCK - 1) // ROW_BLOCK * ROW_BLOCK
    pad_ends = jnp.cumsum(padded)
    dest_pos = pad_ends[sorted_exp] - padded[sorted_exp] + jnp.arange(n_slots, dtype=jnp.int32) - exp_starts[sorted_exp]
    slot_at = jnp.full((n_blocks * ROW_BLOCK,), n_slots, jnp.int32).at[dest_pos].set(order)
    filled = slot_at < n_slots
    safe_slot = jnp.where(filled, slot_at, 0)
    tok_at = safe_slot // TOP_K
    gate_at = jnp.where(filled, route_gate.reshape(n_slots)[safe_slot], 0.0)
    rows = jnp.where(filled[:, None], x[tok_at], 0)
    out_cot = (gate_at[:, None] * grad_y[tok_at].astype(jnp.float32)).astype(jnp.bfloat16)
    block_exp = jnp.minimum(jnp.searchsorted(pad_ends, jnp.arange(n_blocks, dtype=jnp.int32) * ROW_BLOCK, side="right"), GROUP_SIZE - 1)

    def block_step(carry, item):
        acc_gate, acc_up, acc_down = carry
        expert, blk_rows, blk_cot = item
        blk_out, blk_grad, gate_part, up_part, down_part = expert_block(blk_rows, blk_cot, w_gate[expert], w_up[expert], w_down[expert])
        carry = (acc_gate.at[expert].add(gate_part), acc_up.at[expert].add(up_part), acc_down.at[expert].add(down_part))
        return carry, (blk_out, blk_grad)

    init = (jnp.zeros((GROUP_SIZE, D_MODEL, D_FF), jnp.float32), jnp.zeros((GROUP_SIZE, D_MODEL, D_FF), jnp.float32), jnp.zeros((GROUP_SIZE, D_FF, D_MODEL), jnp.float32))
    blocks_in = (block_exp, rows.reshape(n_blocks, ROW_BLOCK, D_MODEL), out_cot.reshape(n_blocks, ROW_BLOCK, D_MODEL))
    (acc_gate, acc_up, acc_down), (outs, grads) = lax.scan(block_step, init, blocks_in)
    outs = outs.reshape(n_blocks * ROW_BLOCK, D_MODEL)
    grads = grads.reshape(n_blocks * ROW_BLOCK, D_MODEL)
    y = jax.ops.segment_sum(gate_at[:, None] * outs.astype(jnp.float32), tok_at, num_segments=T_ALL)
    grad_x = jax.ops.segment_sum(grads.astype(jnp.float32), tok_at, num_segments=T_ALL)
    return (y.astype(jnp.bfloat16), grad_x.astype(jnp.bfloat16), acc_gate.astype(jnp.bfloat16), acc_up.astype(jnp.bfloat16), acc_down.astype(jnp.bfloat16))
```

```python
import jax
import jax.numpy as jnp
from jax import lax
from jax.sharding import PartitionSpec as P

F32 = jnp.float32
BF16 = jnp.bfloat16


class Grid:
    def __init__(self, mesh, cores=2):
        self.count = mesh.shape["ep"]
        self.cores = cores
        self.side = round((self.count // cores) ** 0.5)
        self.me = lax.axis_index("ep")

    def split(self, j):
        return j // (self.cores * self.side), j // self.cores % self.side, j % self.cores

    def join(self, row, col, core):
        return (row % self.side * self.side + col % self.side) * self.cores + core % self.cores

    def shift(self, a, row=0, col=0, core=0):
        pairs = []
        for j in range(self.count):
            r, c, k = self.split(j)
            pairs.append((j, self.join(r + row, c + col, k + core)))
        return lax.ppermute(a, "ep", pairs)


def ring_gather(send, a):
    half = a.shape[0] // 2
    prev = send(a, 1)
    succ = send(a, -1)
    far_top = send(prev[:half], 1)
    far_bottom = send(succ[half:], -1)
    return a, prev, succ, jnp.concatenate([far_top, far_bottom], axis=0)


def ring_reduce(send, own, prev, succ, far):
    half = far.shape[0] // 2
    from_prev = send(far[:half], 1)
    from_succ = send(far[half:], -1)
    succ_rest = send(succ[half:], 1)
    prev_rest = send(prev[:half], -1)
    succ_sum = send(succ[:half] + from_prev, 1)
    prev_sum = send(prev[half:] + from_succ, -1)
    return jnp.concatenate([own[:half] + succ_sum + prev_rest, own[half:] + succ_rest + prev_sum], axis=0)


CONTRACT_LAST = (((1,), (1,)), ((), ()))
CONTRACT_FIRST = (((0,), (0,)), ((), ()))


def dot(a, b, dims=(((1,), (0,)), ((), ()))):
    return lax.dot_general(a, b, dims, preferred_element_type=F32)


def expert_terms(rows, cot, gate, gate_mat, up_mat, down_mat):
    chosen = gate > 0
    pre_gate = dot(rows, gate_mat)
    pre_up = dot(rows, up_mat)
    sig = jax.nn.sigmoid(pre_gate)
    hidden = jnp.where(chosen, pre_gate * sig * pre_up, 0.0).astype(BF16)
    out = dot(hidden, down_mat).astype(BF16)
    y = gate * out.astype(F32)
    scaled = (gate * cot.astype(F32)).astype(BF16)
    grad_hidden = dot(scaled, down_mat, CONTRACT_LAST).astype(BF16).astype(F32)
    grad_gate = jnp.where(chosen, grad_hidden * pre_up * (sig * (1.0 + pre_gate * (1.0 - sig))), 0.0).astype(BF16)
    grad_up = jnp.where(chosen, grad_hidden * (pre_gate * sig), 0.0).astype(BF16)
    grad_rows = (dot(grad_gate, gate_mat, CONTRACT_LAST) + dot(grad_up, up_mat, CONTRACT_LAST)).astype(BF16)
    return y, grad_rows.astype(F32), dot(rows, grad_gate, CONTRACT_FIRST), dot(rows, grad_up, CONTRACT_FIRST), dot(hidden, scaled, CONTRACT_FIRST)


def solution(mesh):
    row_spec = P(("dp", "ep"), None)
    weight_spec = P("ep", None, None)
    grad_w_spec = P(("dp", "ep"), None, None)

    def local(x, route_idx, route_gate, w_gate, w_up, w_down, grad_y):
        grid = Grid(mesh)
        send_col = lambda a, by: grid.shift(a, col=by)
        send_row = lambda a, by: grid.shift(a, row=by)
        swap = lambda a: grid.shift(a, core=1)
        tok = x.shape[0]

        hits = route_idx[:, :, None] == jnp.arange(grid.count, dtype=jnp.int32)[None, None, :]
        gates = jnp.sum(jnp.where(hits, route_gate[:, :, None], 0.0), axis=1).T

        def gather_tokens(a):
            own = ring_gather(send_col, a)
            return jnp.concatenate(own + tuple(swap(b) for b in own), axis=0)

        def gather_gates(a):
            own = (a, send_col(a, 1), send_col(a, -1), send_col(a, 2))
            return jnp.concatenate(own + tuple(swap(b) for b in own), axis=1)

        all_gates = gather_gates(gates)
        mats = [ring_gather(send_row, w[0]) for w in (w_gate, w_up, w_down)]
        rows = gather_tokens(x)
        cot = gather_tokens(grad_y)
        my_row, my_col, my_core = grid.split(grid.me)

        y, grad_x, grads = 0.0, 0.0, [None] * 4
        for slot, step in ((2, 1), (1, -1), (3, 2), (0, 0)):
            expert = grid.join(my_row + step + grid.side, my_col, my_core)
            gate = lax.dynamic_index_in_dim(all_gates, expert, 0, keepdims=False)[:, None]
            y_term, grad_term, *grads[slot] = expert_terms(rows, cot, gate, *(m[slot] for m in mats))
            y = y + y_term
            grad_x = grad_x + grad_term

        def reduce_tokens(a):
            mine = a[: 4 * tok] + swap(a[4 * tok :])
            own, prev, succ, far = (mine[i * tok : (i + 1) * tok] for i in range(4))
            return ring_reduce(send_col, own, prev, succ, far).astype(BF16)

        y = reduce_tokens(y)
        grad_x = reduce_tokens(grad_x)
        grad_w = [ring_reduce(send_row, *(grads[s][i] for s in range(4))).astype(BF16)[None] for i in range(3)]
        return y, grad_x, *grad_w

    return jax.shard_map(local, mesh=mesh, in_specs=(row_spec, row_spec, row_spec, weight_spec, weight_spec, weight_spec, row_spec), out_specs=(row_spec, row_spec, grad_w_spec, grad_w_spec, grad_w_spec), check_vma=False)
```

```python
import functools

import jax
import jax.numpy as jnp
from jax import lax
from jax.experimental import pallas as pl
from jax.experimental.pallas import tpu as pltpu
from jax.sharding import PartitionSpec as P

F32 = jnp.float32
BF16 = jnp.bfloat16


class Grid:
    def __init__(self, mesh, cores=2):
        self.count = mesh.shape["ep"]
        self.cores = cores
        self.side = round((self.count // cores) ** 0.5)
        self.me = lax.axis_index("ep")

    def split(self, j):
        return j // (self.cores * self.side), j // self.cores % self.side, j % self.cores

    def join(self, row, col, core):
        return (row % self.side * self.side + col % self.side) * self.cores + core % self.cores

    def shift(self, a, row=0, col=0, core=0):
        pairs = []
        for j in range(self.count):
            r, c, k = self.split(j)
            pairs.append((j, self.join(r + row, c + col, k + core)))
        return lax.ppermute(a, "ep", pairs)


def ring_gather(send, a):
    half = a.shape[0] // 2
    prev = send(a, 1)
    succ = send(a, -1)
    far_top = send(prev[:half], 1)
    far_bottom = send(succ[half:], -1)
    return a, prev, succ, jnp.concatenate([far_top, far_bottom], axis=0)


def ring_reduce(send, own, prev, succ, far):
    from_prev = send(far[0], 1)
    from_succ = send(far[1], -1)
    succ_rest = send(succ[1], 1)
    prev_rest = send(prev[0], -1)
    succ_sum = send(succ[0] + from_prev, 1)
    prev_sum = send(prev[1] + from_succ, -1)
    return jnp.concatenate([own[0] + succ_sum + prev_rest, own[1] + succ_rest + prev_sum], axis=0)


CONTRACT_LAST = (((1,), (1,)), ((), ()))
CONTRACT_FIRST = (((0,), (0,)), ((), ()))
ALIGN = 16
PART = 128
TILE = 256


def dot(a, b, dims=(((1,), (0,)), ((), ()))):
    return lax.dot_general(a, b, dims, preferred_element_type=F32)


def expert_kernel(first, n_out, n_blocks, block, capacity, count_ref, start_ref, *refs):
    rows_ref, cot_ref, rank_row_ref, gate_row_ref, rank_col_ref, gate_col_ref, wg_ref, wu_ref, wd_ref = refs[:9]
    refs = refs[9:]
    if not first:
        y_in_ref, gx_in_ref = refs[:2]
        refs = refs[2:]
    y_outs, gx_outs, refs = refs[:n_out], refs[n_out : 2 * n_out], refs[2 * n_out :]
    grad_outs, refs = refs[:6], refs[6:]
    xs, cs, acc_g, acc_u, acc_d, stage_y, stage_g, out_sem, grad_sem = refs
    step = pl.program_id(0)
    n_steps = pl.num_programs(0)
    sub = stage_y.shape[1]
    halves = block // sub

    def grad_copies():
        for i, acc in enumerate((acc_g, acc_u, acc_d)):
            half = acc.shape[0] // 2
            for j in range(2):
                yield pltpu.make_async_copy(acc.at[pl.ds(j * half, half)], grad_outs[2 * i + j], grad_sem.at[2 * i + j])

    @pl.when(step < n_blocks)
    def _():
        n = count_ref[step]
        base = start_ref[step]
        rank = rank_row_ref[0]
        gate = gate_row_ref[0]

        def pack(part, carry):
            first_row = part * PART
            ids = lax.broadcasted_iota(jnp.int32, (PART, block), 0) + first_row
            hit = rank == ids
            pick = hit.astype(F32).astype(BF16)
            row_gate = jnp.sum(jnp.where(hit, gate, 0.0), axis=1, keepdims=True)
            at = pl.ds(pl.multiple_of(base + first_row, ALIGN), PART)
            xs[at, :] = dot(pick, rows_ref[...]).astype(BF16)
            cs[at, :] = (row_gate * dot(pick, cot_ref[...])).astype(BF16)
            return carry

        lax.fori_loop(0, (n + PART - 1) // PART, pack, 0)

    @pl.when(step == n_blocks - 1)
    def _():
        total = start_ref[n_blocks]
        slack = max(capacity, TILE)
        at = pl.ds(pl.multiple_of(total, ALIGN), slack)
        xs[at, :] = jnp.zeros((slack, xs.shape[1]), BF16)
        cs[at, :] = jnp.zeros((slack, cs.shape[1]), BF16)
        acc_g[...] = jnp.zeros(acc_g.shape, F32)
        acc_u[...] = jnp.zeros(acc_u.shape, F32)
        acc_d[...] = jnp.zeros(acc_d.shape, F32)

        def run(tile, carry):
            at = pl.ds(pl.multiple_of(tile * TILE, TILE), TILE)
            x = xs[at, :]
            c = cs[at, :]
            a = dot(x, wg_ref[...])
            b = dot(x, wu_ref[...])
            sig = 1.0 / (1.0 + jnp.exp(-a))
            act = a * sig
            h = (act * b).astype(BF16)
            dh = dot(c, wd_ref[...], CONTRACT_LAST).astype(BF16).astype(F32)
            da = (dh * b * (sig * (1.0 + a * (1.0 - sig)))).astype(BF16)
            db = (dh * act).astype(BF16)
            acc_g[...] += dot(x, da, CONTRACT_FIRST)
            acc_u[...] += dot(x, db, CONTRACT_FIRST)
            acc_d[...] += dot(h, c, CONTRACT_FIRST)
            xs[at, :] = dot(h, wd_ref[...]).astype(BF16)
            cs[at, :] = (dot(da, wg_ref[...], CONTRACT_LAST) + dot(db, wu_ref[...], CONTRACT_LAST)).astype(BF16)
            return carry

        lax.fori_loop(0, (total + TILE - 1) // TILE, run, 0)
        for copy in grad_copies():
            copy.start()

    @pl.when(step >= n_blocks)
    def _():
        k = step - n_blocks
        slot = lax.rem(k, 2)
        blk = k // halves
        n = count_ref[blk]
        base = pl.multiple_of(start_ref[blk], ALIGN)
        rank = rank_col_ref[...]
        gate = gate_col_ref[...]

        def out_copies(k, slot, act):
            blk = k // halves
            if n_out == 1:
                act(pltpu.make_async_copy(stage_y.at[slot], y_outs[0].at[pl.ds(pl.multiple_of(k * sub, sub), sub)], out_sem.at[0, slot]))
                act(pltpu.make_async_copy(stage_g.at[slot], gx_outs[0].at[pl.ds(pl.multiple_of(k * sub, sub), sub)], out_sem.at[1, slot]))
                return
            for j in range(n_out):
                @pl.when(k == j)
                def _():
                    act(pltpu.make_async_copy(stage_y.at[slot], y_outs[j], out_sem.at[0, slot]))
                    act(pltpu.make_async_copy(stage_g.at[slot], gx_outs[j], out_sem.at[1, slot]))

        @pl.when(k >= 2)
        def _():
            out_copies(k - 2, slot, lambda copy: copy.wait())

        def scatter(width):
            ids = lax.broadcasted_iota(jnp.int32, (sub, width), 1)
            place = (rank == ids).astype(F32).astype(BF16)
            at = pl.ds(base, width)
            y = gate * dot(place, xs[at, :])
            gx = dot(place, cs[at, :])
            if not first:
                y = y_in_ref[...] + y
                gx = gx_in_ref[...] + gx
            stage_y[slot] = y
            stage_g[slot] = gx

        @pl.when(n <= PART)
        def _():
            scatter(PART)

        @pl.when(n > PART)
        def _():
            scatter(capacity)

        out_copies(k, slot, lambda copy: copy.start())

    @pl.when(step == n_steps - 1)
    def _():
        last = n_steps - 1 - n_blocks
        for k in (last - 1, last):
            slot = lax.rem(k, 2)
            if n_out == 1:
                pltpu.make_async_copy(stage_y.at[slot], y_outs[0].at[pl.ds(0, sub)], out_sem.at[0, slot]).wait()
                pltpu.make_async_copy(stage_g.at[slot], gx_outs[0].at[pl.ds(0, sub)], out_sem.at[1, slot]).wait()
            else:
                pltpu.make_async_copy(stage_y.at[slot], y_outs[0], out_sem.at[0, slot]).wait()
                pltpu.make_async_copy(stage_g.at[slot], gx_outs[0], out_sem.at[1, slot]).wait()
        for copy in grad_copies():
            copy.wait()


def run_expert(rows, cot, meta, mats, sums, n_blocks, capacity, split_out):
    count, start, rank, gate = meta
    n_rows, width = rows.shape
    depth = mats[0].shape[1]
    block = n_rows // n_blocks
    sub = block // 2
    n_sub = n_rows // sub
    first = sums is None
    n_out = n_sub if split_out else 1
    gather_at = lambda i, *_: (jnp.minimum(i, n_blocks - 1), 0)
    gather_at3 = lambda i, *_: (jnp.minimum(i, n_blocks - 1), 0, 0)
    scatter_at = lambda i, *_: (jnp.maximum(i - n_blocks, 0), 0)
    whole = lambda m: pl.BlockSpec(m.shape, lambda i, *_: (0, 0), pipeline_mode=pl.Buffered(1))
    any_spec = pl.BlockSpec(memory_space=pl.ANY)
    in_specs = [pl.BlockSpec((block, width), gather_at)] * 2
    in_specs += [pl.BlockSpec((1, 1, block), gather_at3)] * 2
    in_specs += [pl.BlockSpec((sub, 1), scatter_at)] * 2
    in_specs += [whole(m) for m in mats]
    args = [rows, cot, rank.reshape(n_blocks, 1, block), gate.reshape(n_blocks, 1, block), rank.reshape(n_rows, 1), gate.reshape(n_rows, 1), *mats]
    if not first:
        in_specs += [pl.BlockSpec((sub, width), scatter_at)] * 2
        args += list(sums)
    sum_shape = jax.ShapeDtypeStruct((n_rows // n_out, width), F32)
    outs = [sum_shape] * (2 * n_out)
    for m in mats:
        outs += [jax.ShapeDtypeStruct((m.shape[0] // 2, m.shape[1]), F32)] * 2
    packed = n_blocks * capacity + max(capacity, TILE)
    result = pl.pallas_call(
        functools.partial(expert_kernel, first, n_out, n_blocks, block, capacity),
        out_shape=outs,
        grid_spec=pltpu.PrefetchScalarGridSpec(
            num_scalar_prefetch=2,
            grid=(n_blocks + n_sub,),
            in_specs=in_specs,
            out_specs=[any_spec] * len(outs),
            scratch_shapes=[
                pltpu.VMEM((packed, width), BF16),
                pltpu.VMEM((packed, width), BF16),
                pltpu.VMEM(mats[0].shape, F32),
                pltpu.VMEM(mats[1].shape, F32),
                pltpu.VMEM(mats[2].shape, F32),
                pltpu.VMEM((2, sub, width), F32),
                pltpu.VMEM((2, sub, width), F32),
                pltpu.SemaphoreType.DMA((2, 2)),
                pltpu.SemaphoreType.DMA((6,)),
            ],
        ),
        compiler_params=pltpu.CompilerParams(dimension_semantics=("arbitrary",), vmem_limit_bytes=67043328),
        cost_estimate=pl.CostEstimate(flops=n_rows // 2 * width * depth * 18, bytes_accessed=n_rows * width * 20, transcendentals=n_rows * depth),
    )(count, start, *args)
    y, gx, grads = result[:n_out], result[n_out : 2 * n_out], result[2 * n_out :]
    return y, gx, [grads[2 * i : 2 * i + 2] for i in range(3)]


def solution(mesh):
    row_spec = P(("dp", "ep"), None)
    weight_spec = P("ep", None, None)
    grad_w_spec = P(("dp", "ep"), None, None)

    def local(x, route_idx, route_gate, w_gate, w_up, w_down, grad_y):
        grid = Grid(mesh)
        send_col = lambda a, by: grid.shift(a, col=by)
        send_row = lambda a, by: grid.shift(a, row=by)
        swap = lambda a: grid.shift(a, core=1)
        tok = x.shape[0]
        capacity = 3 * tok // 4
        n_blocks = grid.side * grid.cores

        hits = route_idx[:, :, None] == jnp.arange(grid.count, dtype=jnp.int32)[None, None, :]
        gates = jnp.sum(jnp.where(hits, route_gate[:, :, None], 0.0), axis=1).T

        def gather_tokens(a):
            own = ring_gather(send_col, a)
            return jnp.concatenate(own + tuple(swap(b) for b in own), axis=0)

        own_gates = (gates, send_col(gates, 1), send_col(gates, -1), send_col(gates, 2))
        all_gates = jnp.stack(own_gates + tuple(swap(b) for b in own_gates), axis=1)
        my_row, my_col, my_core = grid.split(grid.me)
        experts = jnp.stack([grid.join(my_row + step + grid.side, my_col, my_core) for step in (0, -1, 1, 2)])
        gate = jnp.take(all_gates, experts, axis=0)
        chosen = gate > 0
        upto = (jnp.arange(tok)[:, None] <= jnp.arange(tok)[None, :]).astype(BF16)
        rank = dot(chosen.reshape(-1, tok).astype(BF16), upto).astype(jnp.int32).reshape(gate.shape) - 1
        count = rank[:, :, -1] + 1
        rank = jnp.where(chosen, rank, -1)
        padded = (count + ALIGN - 1) // ALIGN * ALIGN
        start = jnp.concatenate([jnp.zeros_like(padded[:, :1]), jnp.cumsum(padded, axis=1)], axis=1)

        mats = [ring_gather(send_row, w[0]) for w in (w_gate, w_up, w_down)]
        rows = gather_tokens(x)
        cot = gather_tokens(grad_y)

        sums, grads = None, [None] * 4
        for i, slot in enumerate((2, 1, 3, 0)):
            meta = (count[slot], start[slot], rank[slot], gate[slot])
            y, grad_x, grads[slot] = run_expert(rows, cot, meta, [m[slot] for m in mats], sums, n_blocks, capacity, i == 3)
            sums = None if i == 3 else (y[0], grad_x[0])

        def reduce_tokens(parts):
            mine = {}
            for blk in (3, 2, 1, 0):
                mine[blk] = [parts[2 * blk + j] + swap(parts[2 * (grid.side + blk) + j]) for j in range(2)]
            return ring_reduce(send_col, mine[0], mine[1], mine[2], mine[3]).astype(BF16)

        y = reduce_tokens(y)
        grad_x = reduce_tokens(grad_x)
        grad_w = [ring_reduce(send_row, *(grads[s][i] for s in range(4))).astype(BF16)[None] for i in range(3)]
        return y, grad_x, *grad_w

    return jax.shard_map(local, mesh=mesh, in_specs=(row_spec, row_spec, row_spec, weight_spec, weight_spec, weight_spec, row_spec), out_specs=(row_spec, row_spec, grad_w_spec, grad_w_spec, grad_w_spec), check_vma=False)
```
